32 devices in a mesh: grp: 2 (over core), ex: 16 (over z, y, x).
Axes of the slice: x: 2, y: 2, z: 4, core: 2. Of those that a mesh axis runs over, the one named last changes fastest.
Arguments:
- tokens: bfloat16 [8192, 1024], P(('grp', 'ex')), may hold values from -6 to 6
- expert_ids: int32 [8192], P(('grp', 'ex')), may hold values from 0 to 15, as said below
- slot_ids: int32 [8192], P(('grp', 'ex')), may hold values from 0 to 31, as said below
- centroids: bfloat16 [16, 1024], replicated, may hold values from -0.1875 to 0.1875
- w_in: bfloat16 [16, 1024, 4096], P('ex', None, 'grp'), may hold values from -0.1875 to 0.1875
- w_out: bfloat16 [16, 4096, 1024], P('ex', 'grp'), may hold values from -0.09375 to 0.09375
Outputs:
- combined: bfloat16 [8192, 1024], P(('grp', 'ex'))
The draws below stay inside these ranges and needn't reach their ends.
Inputs may be any that keep to these rules, and one draw needn't show every extreme that they name: `expert_ids`: within each device's 256 rows, at most 32 rows name one expert; in every device some expert is named by exactly 32 rows, and in each group of 16 devices along ex one expert is named by 32 rows on every device of the group. `slot_ids`: rows of one device that name the same expert have distinct slots.
All inputs are finite; a program needn't handle non-finite values.
Results may differ from the reference program's by a relative error of at most 0.0035.
Values may be sent and summed in bfloat16 or wider, within the bound.
A program may use at most 128 MiB of HBM per device.

```python
import jax
import jax.numpy as jnp
from jax import lax

D = 1024
FF = 4096
TOK_DEV = 256
EXPERTS = 16
TOKENS = 8192
CAP = 32


def assignment(key):
    base_key = jax.random.fold_in(key, 11)
    group_count = TOKENS // (TOK_DEV * EXPERTS)
    hot_experts = jax.random.randint(jax.random.fold_in(base_key, 1), (group_count,), 0, EXPERTS)
    block_keys = jax.random.split(jax.random.fold_in(base_key, 2), TOKENS // TOK_DEV)
    hot_list = jnp.repeat(hot_experts, EXPERTS)

    def one_block(block_key, hot_one):
        key_full, key_perm, key_rows = jax.random.split(block_key, 3)
        favoured = jax.random.randint(key_full, (), 0, EXPERTS)
        shuffled = jax.random.permutation(key_perm, EXPERTS * CAP).astype(jnp.int32)
        owner = shuffled // CAP
        classes = jnp.where(owner == hot_one, 0, jnp.where(owner == favoured, 1, 2)).astype(jnp.int32)
        ordering = jnp.argsort(classes * (EXPERTS * CAP) + jnp.arange(EXPERTS * CAP, dtype=jnp.int32))
        picked = shuffled[ordering][:TOK_DEV]
        picked = picked[jax.random.permutation(key_rows, TOK_DEV)]
        return (picked // CAP, picked % CAP)
    owners, places = jax.vmap(one_block)(block_keys, hot_list)
    return (owners.reshape(-1).astype(jnp.int32), places.reshape(-1).astype(jnp.int32))


def draw_expert_ids(key, part):
    return assignment(key)[0]


def draw_slot_ids(key, part):
    return assignment(key)[1]


def level_of(key, extent, shards, least, largest):
    def one(position, parts):
        draws = jax.random.uniform(jax.random.fold_in(jax.random.fold_in(key, 6), position), (parts,), jnp.float32, least / len(shards), largest / len(shards))
        return jnp.repeat(jnp.exp(draws), extent[position] // parts).reshape((-1,) + (1,) * (len(extent) - position - 1))

    gain = one(*shards[0])
    for cut in shards[1:]:
        gain = gain * one(*cut)
    return gain


def scatter_about(stream_key, dims, scale, reach, pieces=(), held_as=jnp.bfloat16):
    result = scale * jax.random.normal(stream_key, dims, jnp.float32)
    if pieces:
        result = result * level_of(stream_key, dims, pieces, -0.22, 0.18)
    return jnp.clip(result, -reach, reach).astype(held_as)


def setup_inputs(seed: int = 0) -> dict:
    keys = jax.random.split(jax.random.key(seed), 7)
    tokens = scatter_about(keys[0], (TOKENS, D), 1.0, 6.0, ((0, 32),))
    expert_ids = draw_expert_ids(jax.random.fold_in(keys[6], 71), 0)
    slot_ids = draw_slot_ids(jax.random.fold_in(keys[6], 71), 0)
    centroids = scatter_about(keys[3], (EXPERTS, D), D ** -0.5, 0.1875)
    w_in = scatter_about(keys[4], (EXPERTS, D, FF), D ** -0.5, 0.1875, ((0, 16), (2, 2)))
    w_out = scatter_about(keys[5], (EXPERTS, FF, D), FF ** -0.5, 0.09375, ((0, 16), (1, 2)))
    return {"tokens": tokens, "expert_ids": expert_ids, "slot_ids": slot_ids, "centroids": centroids, "w_in": w_in, "w_out": w_out}


def reference(tokens, expert_ids, slot_ids, centroids, w_in, w_out):
    block_count = TOKENS // TOK_DEV
    block_ids = jnp.arange(TOKENS, dtype=jnp.int32) // TOK_DEV
    buffer_rows = (expert_ids * (block_count * CAP) + block_ids * CAP + slot_ids).astype(jnp.int32)
    total_rows = EXPERTS * block_count * CAP
    buffer = jnp.zeros((total_rows, D), jnp.bfloat16).at[buffer_rows].set(tokens)
    buffer = buffer.reshape(EXPERTS, block_count * CAP, D)

    def expert(operands):
        rows_in, first, second = operands
        hidden = jnp.maximum(jnp.dot(rows_in, first, preferred_element_type=jnp.float32), 0.0).astype(jnp.bfloat16)
        return jnp.dot(hidden, second, preferred_element_type=jnp.float32).astype(jnp.bfloat16)

    results = lax.map(expert, (buffer, w_in, w_out)).reshape(total_rows, D)
    arrived = results[buffer_rows]
    scores = jnp.dot(tokens, centroids.T, preferred_element_type=jnp.float32)
    columns = jnp.arange(EXPERTS, dtype=jnp.int32)
    chosen = jnp.sum(jnp.where(columns[None, :] == expert_ids[:, None], scores, 0.0), axis=1)
    gating = jax.nn.sigmoid(chosen)
    return (tokens.astype(jnp.float32) + gating[:, None] * arrived.astype(jnp.float32)).astype(jnp.bfloat16)
```

```python
import functools

import jax
import jax.numpy as jnp
from jax import lax
from jax.experimental import pallas as pl
from jax.experimental.pallas import tpu as pltpu
from jax.sharding import PartitionSpec as P

MESH = pl.DeviceIdType.MESH
TILE = 512


def expert_kernel(
    n,
    cap,
    ids_ref,
    slots_ref,
    tokens_ref,
    centroids_ref,
    w_in_ref,
    w_out_ref,
    out_ref,
    outgoing,
    received,
    result,
    returned,
    total,
    place,
    columns,
    full_in,
    full_out,
    load_sem,
    share_send,
    share_recv,
    send_sem,
    recv_sem,
    back_send,
    back_recv,
):
    grp = lax.axis_index("grp")
    me = lax.axis_index("ex")
    half = n // 2
    side = me // half
    seat = me % half
    quarter = n // 4
    rows = quarter * cap
    tokens_here, width = tokens_ref.shape
    hidden = full_in.shape[2]

    def peer_to(slot):
        return ((side + slot // half) % 2) * half + (seat + slot % half) % half

    def peer_from(slot):
        return ((side + slot // half) % 2) * half + (seat + half - slot % half) % half

    def block(slot):
        start = slot * cap
        if not isinstance(slot, int):
            start = pl.multiple_of(start, cap)
        return pl.ds(start, cap)

    barrier = pltpu.get_barrier_semaphore()
    for slot in range(1, n):
        pl.semaphore_signal(
            barrier, inc=1, device_id={"ex": peer_to(slot)}, device_id_type=MESH
        )
    pl.semaphore_signal(barrier, inc=1, device_id={"grp": 1 - grp}, device_id_type=MESH)

    loads = [
        pltpu.make_async_copy(w_in_ref.at[0], full_in.at[0], load_sem.at[0]),
        pltpu.make_async_copy(w_out_ref.at[0], full_out.at[0], load_sem.at[1]),
    ]
    for load in loads:
        load.start()

    ids = ids_ref[...]
    high = (ids >= half).astype(jnp.int32)
    ahead = ids - high * half - seat
    ahead = jnp.where(ahead < 0, ahead + half, ahead)
    across = jnp.where(high == side, 0, 1)
    position = (across * half + ahead) * cap + slots_ref[...]
    slot_rows = lax.broadcasted_iota(jnp.int32, (n * cap, tokens_here), 0)
    spread = (slot_rows == position).astype(jnp.bfloat16)
    packed = jnp.dot(spread, tokens_ref[...], preferred_element_type=jnp.float32)
    packed = packed.astype(jnp.bfloat16)
    outgoing[...] = packed
    received[block(0), :] = packed[:cap]

    shares = [
        pltpu.make_async_remote_copy(
            src_ref=w_in_ref.at[0],
            dst_ref=full_in.at[1],
            send_sem=share_send.at[0],
            recv_sem=share_recv.at[0],
            device_id={"grp": 1 - grp},
            device_id_type=MESH,
        ),
        pltpu.make_async_remote_copy(
            src_ref=w_out_ref.at[0],
            dst_ref=full_out.at[1],
            send_sem=share_send.at[1],
            recv_sem=share_recv.at[1],
            device_id={"grp": 1 - grp},
            device_id_type=MESH,
        ),
    ]

    def dispatch(slot):
        return pltpu.make_async_remote_copy(
            src_ref=outgoing.at[block(slot), :],
            dst_ref=received.at[block(slot), :],
            send_sem=send_sem.at[slot],
            recv_sem=recv_sem.at[slot],
            device_id={"ex": peer_to(slot)},
            device_id_type=MESH,
        )

    def give_back(slot):
        return pltpu.make_async_remote_copy(
            src_ref=result.at[block(slot), :],
            dst_ref=returned.at[block(slot), :],
            send_sem=back_send.at[slot],
            recv_sem=back_recv.at[slot],
            device_id={"ex": peer_from(slot)},
            device_id_type=MESH,
        )

    pl.semaphore_wait(barrier, n)
    for step in range(half):
        dispatch(half + step).start()
        if step > 0:
            dispatch(step).start()
    for share in shares:
        share.start()

    scores = lax.dot_general(
        centroids_ref[...],
        tokens_ref[...],
        (((1,), (1,)), ((), ())),
        preferred_element_type=jnp.float32,
    )
    experts = lax.broadcasted_iota(jnp.int32, scores.shape, 0)
    chosen = jnp.sum(jnp.where(experts == ids, scores, 0.0), axis=0, keepdims=True)
    gating = 1.0 / (1.0 + jnp.exp(-chosen))
    lines = lax.broadcasted_iota(jnp.int32, (128, tokens_here), 0)
    columns[...] = jnp.where(lines == 0, position.astype(jnp.float32), gating).T
    slot_columns = lax.broadcasted_iota(jnp.int32, (tokens_here, n * cap), 1)
    place[...] = (slot_columns == columns[:, 0:1].astype(jnp.int32)).astype(jnp.bfloat16)

    for load in loads:
        load.wait()
    for share in shares:
        share.wait_recv()

    @pl.loop(0, 4)
    def _(turn):
        chunk = (2 + 2 * turn) % 4 + turn // 2
        first = chunk * quarter

        @pl.loop(0, quarter)
        def _(k):
            @pl.when(first + k > 0)
            def _():
                dispatch(first + k).wait_recv()

        here = pl.ds(pl.multiple_of(chunk * rows, rows), rows)
        total[...] = jnp.zeros_like(total)

        @pl.loop(0, 2 * (hidden // TILE))
        def _(piece):
            part = piece // (hidden // TILE)
            cut = pl.ds(pl.multiple_of((piece % (hidden // TILE)) * TILE, TILE), TILE)
            middle = jnp.dot(
                received[here, :], full_in[part, :, cut], preferred_element_type=jnp.float32
            )
            middle = jnp.maximum(middle, 0.0).astype(jnp.bfloat16)
            total[...] += jnp.dot(
                middle, full_out[part, cut, :], preferred_element_type=jnp.float32
            )

        result[here, :] = total[...].astype(jnp.bfloat16)

        @pl.loop(0, quarter)
        def _(k):
            @pl.when(first + k > 0)
            def _():
                give_back(first + k).start()

            @pl.when(first + k == 0)
            def _():
                returned[block(0), :] = result[block(0), :]

    arrived = jnp.zeros((tokens_here, width), jnp.float32)
    for chunk in range(4):
        for slot in range(chunk * quarter, (chunk + 1) * quarter):
            if slot > 0:
                give_back(slot).wait_recv()
        here = pl.ds(chunk * rows, rows)
        arrived += jnp.dot(
            place[:, here], returned[here, :], preferred_element_type=jnp.float32
        )
    mixed = tokens_ref[...].astype(jnp.float32) + columns[:, 1:2] * arrived
    out_ref[...] = mixed.astype(jnp.bfloat16)

    @pl.loop(1, n)
    def _(slot):
        dispatch(slot).wait_send()
        give_back(slot).wait_send()

    for share in shares:
        share.wait_send()


def in_one_kernel(n, tokens, expert_ids, slot_ids, centroids, w_in, w_out):
    count, width = tokens.shape
    cap = 2 * count // n
    slots = n * cap
    rows = slots // 4
    hidden = w_in.shape[2]
    vmem = pl.BlockSpec(memory_space=pltpu.VMEM)
    hbm = pl.BlockSpec(memory_space=pl.ANY)
    sems = pltpu.SemaphoreType.DMA
    return pl.pallas_call(
        functools.partial(expert_kernel, n, cap),
        out_shape=jax.ShapeDtypeStruct((count, width), jnp.bfloat16),
        in_specs=[vmem, vmem, vmem, vmem, hbm, hbm],
        out_specs=vmem,
        scratch_shapes=[
            pltpu.VMEM((slots, width), jnp.bfloat16),
            pltpu.VMEM((slots, width), jnp.bfloat16),
            pltpu.VMEM((slots, width), jnp.bfloat16),
            pltpu.VMEM((slots, width), jnp.bfloat16),
            pltpu.VMEM((rows, width), jnp.float32),
            pltpu.VMEM((count, slots), jnp.bfloat16),
            pltpu.VMEM((count, 128), jnp.float32),
            pltpu.VMEM((2, width, hidden), jnp.bfloat16),
            pltpu.VMEM((2, hidden, width), jnp.bfloat16),
            sems((2,)),
            sems((2,)),
            sems((2,)),
            sems((n,)),
            sems((n,)),
            sems((n,)),
            sems((n,)),
        ],
        compiler_params=pltpu.CompilerParams(
            collective_id=0, has_side_effects=True, vmem_limit_bytes=60 * 1024 * 1024
        ),
    )(
        expert_ids.reshape(1, count),
        slot_ids.reshape(1, count),
        tokens,
        centroids,
        w_in,
        w_out,
    )


def in_plain_ops(tokens, expert_ids, slot_ids, centroids, w_in, w_out):
    experts = centroids.shape[0]
    count_rows = tokens.shape[0]
    model_width = tokens.shape[1]
    capacity = 2 * count_rows // experts
    buffer_rows = expert_ids * capacity + slot_ids
    outgoing = (
        jnp.zeros((experts * capacity, model_width), jnp.bfloat16).at[buffer_rows].set(tokens)
    )
    outgoing = outgoing.reshape(experts, capacity, model_width)
    scores = jnp.dot(tokens, centroids.T, preferred_element_type=jnp.float32)
    columns = jnp.arange(experts, dtype=jnp.int32)
    chosen = jnp.sum(jnp.where(columns[None, :] == expert_ids[:, None], scores, 0.0), axis=1)
    gating = jax.nn.sigmoid(chosen)
    full_in, full_out = (
        lax.all_gather(w_in, "grp", axis=2, tiled=True),
        lax.all_gather(w_out, "grp", axis=1, tiled=True),
    )
    received = lax.all_to_all(outgoing, "ex", split_axis=0, concat_axis=0, tiled=True)
    flat_rows = received.reshape(-1, model_width)
    hidden = jnp.maximum(
        jnp.dot(flat_rows, full_in[0], preferred_element_type=jnp.float32), 0.0
    ).astype(jnp.bfloat16)
    result = jnp.dot(hidden, full_out[0], preferred_element_type=jnp.float32)
    returned = lax.all_to_all(
        result.astype(jnp.bfloat16).reshape(received.shape),
        "ex",
        split_axis=0,
        concat_axis=0,
        tiled=True,
    )
    arrived = returned.reshape(-1, model_width)[buffer_rows]
    mixed_rows = tokens.astype(jnp.float32) + gating[:, None] * arrived.astype(jnp.float32)
    return mixed_rows.astype(jnp.bfloat16)


def solution(mesh):
    n = mesh.shape["ex"]

    def on_device(tokens, expert_ids, slot_ids, centroids, w_in, w_out):
        capacity = 2 * tokens.shape[0] // n
        if mesh.shape["grp"] == 2 and n % 4 == 0 and capacity % 16 == 0:
            return in_one_kernel(n, tokens, expert_ids, slot_ids, centroids, w_in, w_out)
        return in_plain_ops(tokens, expert_ids, slot_ids, centroids, w_in, w_out)

    in_specs = (
        P(("grp", "ex"), None),
        P(("grp", "ex")),
        P(("grp", "ex")),
        P(),
        P("ex", None, "grp"),
        P("ex", "grp", None),
    )
    out_specs = P(("grp", "ex"), None)
    return jax.shard_map(
        on_device, mesh=mesh, in_specs=in_specs, out_specs=out_specs, check_vma=False
    )
```

```python
import functools

import jax
import jax.numpy as jnp
from jax import lax
from jax.experimental import pallas as pl
from jax.experimental.pallas import tpu as pltpu
from jax.sharding import PartitionSpec as P

MESH = pl.DeviceIdType.MESH
TILE = 1024


def expert_kernel(
    n,
    cap,
    ids_ref,
    slots_ref,
    tokens_ref,
    centroids_ref,
    w_in_ref,
    w_out_ref,
    out_ref,
    outgoing,
    received,
    result,
    returned,
    total,
    place,
    columns,
    full_in,
    full_out,
    load_sem,
    share_send,
    share_recv,
    send_sem,
    recv_sem,
    back_send,
    back_recv,
):
    grp = lax.axis_index("grp")
    me = lax.axis_index("ex")
    half = n // 2
    side = me // half
    seat = me % half
    quarter = n // 4
    rows = quarter * cap
    tokens_here, width = tokens_ref.shape
    hidden = full_in.shape[2]

    def peer_to(slot):
        return ((side + slot // half) % 2) * half + (seat + slot % half) % half

    def peer_from(slot):
        return ((side + slot // half) % 2) * half + (seat + half - slot % half) % half

    def block(slot):
        start = slot * cap
        if not isinstance(slot, int):
            start = pl.multiple_of(start, cap)
        return pl.ds(start, cap)

    barrier = pltpu.get_barrier_semaphore()
    for slot in range(1, n):
        pl.semaphore_signal(
            barrier, inc=1, device_id={"ex": peer_to(slot)}, device_id_type=MESH
        )
    pl.semaphore_signal(barrier, inc=1, device_id={"grp": 1 - grp}, device_id_type=MESH)

    loads = [
        pltpu.make_async_copy(w_in_ref.at[0], full_in.at[0], load_sem.at[0]),
        pltpu.make_async_copy(w_out_ref.at[0], full_out.at[0], load_sem.at[1]),
    ]
    for load in loads:
        load.start()

    ids = ids_ref[...]
    high = (ids >= half).astype(jnp.int32)
    ahead = ids - high * half - seat
    ahead = jnp.where(ahead < 0, ahead + half, ahead)
    across = jnp.where(high == side, 0, 1)
    position = (across * half + ahead) * cap + slots_ref[...]
    slot_rows = lax.broadcasted_iota(jnp.int32, (n * cap, tokens_here), 0)
    spread = (slot_rows == position).astype(jnp.bfloat16)
    packed = jnp.dot(spread, tokens_ref[...], preferred_element_type=jnp.float32)
    packed = packed.astype(jnp.bfloat16)
    outgoing[...] = packed
    received[block(0), :] = packed[:cap]

    shares = [
        pltpu.make_async_remote_copy(
            src_ref=w_in_ref.at[0],
            dst_ref=full_in.at[1],
            send_sem=share_send.at[0],
            recv_sem=share_recv.at[0],
            device_id={"grp": 1 - grp},
            device_id_type=MESH,
        ),
        pltpu.make_async_remote_copy(
            src_ref=w_out_ref.at[0],
            dst_ref=full_out.at[1],
            send_sem=share_send.at[1],
            recv_sem=share_recv.at[1],
            device_id={"grp": 1 - grp},
            device_id_type=MESH,
        ),
    ]

    def dispatch(slot):
        return pltpu.make_async_remote_copy(
            src_ref=outgoing.at[block(slot), :],
            dst_ref=received.at[block(slot), :],
            send_sem=send_sem.at[slot],
            recv_sem=recv_sem.at[slot],
            device_id={"ex": peer_to(slot)},
            device_id_type=MESH,
        )

    def give_back(slot):
        return pltpu.make_async_remote_copy(
            src_ref=result.at[block(slot), :],
            dst_ref=returned.at[block(slot), :],
            send_sem=back_send.at[slot],
            recv_sem=back_recv.at[slot],
            device_id={"ex": peer_from(slot)},
            device_id_type=MESH,
        )

    pl.semaphore_wait(barrier, n)
    for step in reversed(range(half)):
        dispatch(half + step).start()
        if step > 0:
            dispatch(step).start()
    for share in shares:
        share.start()

    scores = lax.dot_general(
        centroids_ref[...],
        tokens_ref[...],
        (((1,), (1,)), ((), ())),
        preferred_element_type=jnp.float32,
    )
    experts = lax.broadcasted_iota(jnp.int32, scores.shape, 0)
    chosen = jnp.sum(jnp.where(experts == ids, scores, 0.0), axis=0, keepdims=True)
    gating = 1.0 / (1.0 + jnp.exp(-chosen))
    lines = lax.broadcasted_iota(jnp.int32, (128, tokens_here), 0)
    columns[...] = jnp.where(lines == 0, position.astype(jnp.float32), gating).T
    slot_columns = lax.broadcasted_iota(jnp.int32, (tokens_here, n * cap), 1)
    place[...] = (slot_columns == columns[:, 0:1].astype(jnp.int32)).astype(jnp.bfloat16)

    for load in loads:
        load.wait()
    for share in shares:
        share.wait_recv()

    @pl.loop(0, 4)
    def _(turn):
        chunk = 3 - (2 * turn) % 4 - turn // 2
        first = chunk * quarter

        @pl.loop(0, quarter)
        def _(k):
            @pl.when(first + k > 0)
            def _():
                dispatch(first + k).wait_recv()

        here = pl.ds(pl.multiple_of(chunk * rows, rows), rows)
        total[...] = jnp.zeros_like(total)

        @pl.loop(0, 2 * (hidden // TILE))
        def _(piece):
            part = piece // (hidden // TILE)
            cut = pl.ds(pl.multiple_of((piece % (hidden // TILE)) * TILE, TILE), TILE)
            middle = jnp.dot(
                received[here, :], full_in[part, :, cut], preferred_element_type=jnp.float32
            )
            middle = jnp.maximum(middle, 0.0).astype(jnp.bfloat16)
            total[...] += jnp.dot(
                middle, full_out[part, cut, :], preferred_element_type=jnp.float32
            )

        result[here, :] = total[...].astype(jnp.bfloat16)

        @pl.loop(0, quarter)
        def _(k):
            @pl.when(first + k > 0)
            def _():
                give_back(first + k).start()

            @pl.when(first + k == 0)
            def _():
                returned[block(0), :] = result[block(0), :]

    arrived = jnp.zeros((tokens_here, width), jnp.float32)
    for chunk in (1, 3, 0, 2):
        for slot in range(chunk * quarter, (chunk + 1) * quarter):
            if slot > 0:
                give_back(slot).wait_recv()
        here = pl.ds(chunk * rows, rows)
        arrived += jnp.dot(
            place[:, here], returned[here, :], preferred_element_type=jnp.float32
        )
    mixed = tokens_ref[...].astype(jnp.float32) + columns[:, 1:2] * arrived
    out_ref[...] = mixed.astype(jnp.bfloat16)

    @pl.loop(1, n)
    def _(slot):
        dispatch(slot).wait_send()
        give_back(slot).wait_send()

    for share in shares:
        share.wait_send()


def in_one_kernel(n, tokens, expert_ids, slot_ids, centroids, w_in, w_out):
    count, width = tokens.shape
    cap = 2 * count // n
    slots = n * cap
    rows = slots // 4
    hidden = w_in.shape[2]
    vmem = pl.BlockSpec(memory_space=pltpu.VMEM)
    hbm = pl.BlockSpec(memory_space=pl.ANY)
    sems = pltpu.SemaphoreType.DMA
    return pl.pallas_call(
        functools.partial(expert_kernel, n, cap),
        out_shape=jax.ShapeDtypeStruct((count, width), jnp.bfloat16),
        in_specs=[vmem, vmem, vmem, vmem, hbm, hbm],
        out_specs=vmem,
        scratch_shapes=[
            pltpu.VMEM((slots, width), jnp.bfloat16),
            pltpu.VMEM((slots, width), jnp.bfloat16),
            pltpu.VMEM((slots, width), jnp.bfloat16),
            pltpu.VMEM((slots, width), jnp.bfloat16),
            pltpu.VMEM((rows, width), jnp.float32),
            pltpu.VMEM((count, slots), jnp.bfloat16),
            pltpu.VMEM((count, 128), jnp.float32),
            pltpu.VMEM((2, width, hidden), jnp.bfloat16),
            pltpu.VMEM((2, hidden, width), jnp.bfloat16),
            sems((2,)),
            sems((2,)),
            sems((2,)),
            sems((n,)),
            sems((n,)),
            sems((n,)),
            sems((n,)),
        ],
        compiler_params=pltpu.CompilerParams(
            collective_id=0, has_side_effects=True, vmem_limit_bytes=60 * 1024 * 1024
        ),
    )(
        expert_ids.reshape(1, count),
        slot_ids.reshape(1, count),
        tokens,
        centroids,
        w_in,
        w_out,
    )


def in_plain_ops(tokens, expert_ids, slot_ids, centroids, w_in, w_out):
    experts = centroids.shape[0]
    count_rows = tokens.shape[0]
    model_width = tokens.shape[1]
    capacity = 2 * count_rows // experts
    buffer_rows = expert_ids * capacity + slot_ids
    outgoing = (
        jnp.zeros((experts * capacity, model_width), jnp.bfloat16).at[buffer_rows].set(tokens)
    )
    outgoing = outgoing.reshape(experts, capacity, model_width)
    scores = jnp.dot(tokens, centroids.T, preferred_element_type=jnp.float32)
    columns = jnp.arange(experts, dtype=jnp.int32)
    chosen = jnp.sum(jnp.where(columns[None, :] == expert_ids[:, None], scores, 0.0), axis=1)
    gating = jax.nn.sigmoid(chosen)
    full_in, full_out = (
        lax.all_gather(w_in, "grp", axis=2, tiled=True),
        lax.all_gather(w_out, "grp", axis=1, tiled=True),
    )
    received = lax.all_to_all(outgoing, "ex", split_axis=0, concat_axis=0, tiled=True)
    flat_rows = received.reshape(-1, model_width)
    hidden = jnp.maximum(
        jnp.dot(flat_rows, full_in[0], preferred_element_type=jnp.float32), 0.0
    ).astype(jnp.bfloat16)
    result = jnp.dot(hidden, full_out[0], preferred_element_type=jnp.float32)
    returned = lax.all_to_all(
        result.astype(jnp.bfloat16).reshape(received.shape),
        "ex",
        split_axis=0,
        concat_axis=0,
        tiled=True,
    )
    arrived = returned.reshape(-1, model_width)[buffer_rows]
    mixed_rows = tokens.astype(jnp.float32) + gating[:, None] * arrived.astype(jnp.float32)
    return mixed_rows.astype(jnp.bfloat16)


def solution(mesh):
    n = mesh.shape["ex"]

    def on_device(tokens, expert_ids, slot_ids, centroids, w_in, w_out):
        capacity = 2 * tokens.shape[0] // n
        if mesh.shape["grp"] == 2 and n % 4 == 0 and capacity % 16 == 0:
            return in_one_kernel(n, tokens, expert_ids, slot_ids, centroids, w_in, w_out)
        return in_plain_ops(tokens, expert_ids, slot_ids, centroids, w_in, w_out)

    in_specs = (
        P(("grp", "ex"), None),
        P(("grp", "ex")),
        P(("grp", "ex")),
        P(),
        P("ex", None, "grp"),
        P("ex", "grp", None),
    )
    out_specs = P(("grp", "ex"), None)
    return jax.shard_map(
        on_device, mesh=mesh, in_specs=in_specs, out_specs=out_specs, check_vma=False
    )
```

```python
import functools

import jax
import jax.numpy as jnp
from jax import lax
from jax.experimental import pallas as pl
from jax.experimental.pallas import tpu as pltpu
from jax.sharding import PartitionSpec as P

MESH = pl.DeviceIdType.MESH
TILE = 1024


def expert_kernel(
    n,
    cap,
    ids_ref,
    slots_ref,
    tokens_hbm,
    centroids_ref,
    w_in_ref,
    w_out_ref,
    out_ref,
    outgoing,
    received,
    result,
    returned,
    total,
    tokens_ref,
    place,
    columns,
    full_in,
    full_out,
    load_sem,
    share_send,
    share_recv,
    send_sem,
    recv_sem,
    back_send,
    back_recv,
):
    grp = lax.axis_index("grp")
    me = lax.axis_index("ex")
    half = n // 2
    side = me // half
    seat = me % half
    quarter = n // 4
    rows = quarter * cap
    tokens_here, width = tokens_ref.shape
    hidden = full_in.shape[2]

    def peer_to(slot):
        return ((side + slot // half) % 2) * half + (seat + slot % half) % half

    def peer_from(slot):
        return ((side + slot // half) % 2) * half + (seat + half - slot % half) % half

    def block(slot):
        start = slot * cap
        if not isinstance(slot, int):
            start = pl.multiple_of(start, cap)
        return pl.ds(start, cap)

    barrier = pltpu.get_barrier_semaphore()
    for slot in range(1, n):
        pl.semaphore_signal(
            barrier, inc=1, device_id={"ex": peer_to(slot)}, device_id_type=MESH
        )
    pl.semaphore_signal(barrier, inc=1, device_id={"grp": 1 - grp}, device_id_type=MESH)

    bring = pltpu.make_async_copy(tokens_hbm, tokens_ref, load_sem.at[2])
    bring.start()
    loads = [
        pltpu.make_async_copy(w_in_ref.at[0], full_in.at[0], load_sem.at[0]),
        pltpu.make_async_copy(w_out_ref.at[0], full_out.at[0], load_sem.at[1]),
    ]
    for load in loads:
        load.start()

    ids = ids_ref[...]
    high = (ids >= half).astype(jnp.int32)
    ahead = ids - high * half - seat
    ahead = jnp.where(ahead < 0, ahead + half, ahead)
    across = jnp.where(high == side, 0, 1)
    position = (across * half + ahead) * cap + slots_ref[...]
    slot_rows = lax.broadcasted_iota(jnp.int32, (n * cap, tokens_here), 0)
    spread = (slot_rows == position).astype(jnp.bfloat16)
    bring.wait()
    packed = jnp.dot(spread, tokens_ref[...], preferred_element_type=jnp.float32)
    packed = packed.astype(jnp.bfloat16)
    outgoing[...] = packed
    received[block(0), :] = packed[:cap]

    shares = [
        pltpu.make_async_remote_copy(
            src_ref=w_in_ref.at[0],
            dst_ref=full_in.at[1],
            send_sem=share_send.at[0],
            recv_sem=share_recv.at[0],
            device_id={"grp": 1 - grp},
            device_id_type=MESH,
        ),
        pltpu.make_async_remote_copy(
            src_ref=w_out_ref.at[0],
            dst_ref=full_out.at[1],
            send_sem=share_send.at[1],
            recv_sem=share_recv.at[1],
            device_id={"grp": 1 - grp},
            device_id_type=MESH,
        ),
    ]

    def dispatch(slot):
        return pltpu.make_async_remote_copy(
            src_ref=outgoing.at[block(slot), :],
            dst_ref=received.at[block(slot), :],
            send_sem=send_sem.at[slot],
            recv_sem=recv_sem.at[slot],
            device_id={"ex": peer_to(slot)},
            device_id_type=MESH,
        )

    def give_back(slot):
        return pltpu.make_async_remote_copy(
            src_ref=result.at[block(slot), :],
            dst_ref=returned.at[block(slot), :],
            send_sem=back_send.at[slot],
            recv_sem=back_recv.at[slot],
            device_id={"ex": peer_from(slot)},
            device_id_type=MESH,
        )

    pl.semaphore_wait(barrier, n)
    for step in reversed(range(half)):
        dispatch(half + step).start()
        if step > 0:
            dispatch(step).start()
    for share in shares:
        share.start()

    scores = lax.dot_general(
        centroids_ref[...],
        tokens_ref[...],
        (((1,), (1,)), ((), ())),
        preferred_element_type=jnp.float32,
    )
    experts = lax.broadcasted_iota(jnp.int32, scores.shape, 0)
    chosen = jnp.sum(jnp.where(experts == ids, scores, 0.0), axis=0, keepdims=True)
    gating = 1.0 / (1.0 + jnp.exp(-chosen))
    lines = lax.broadcasted_iota(jnp.int32, (128, tokens_here), 0)
    columns[...] = jnp.where(lines == 0, position.astype(jnp.float32), gating).T
    slot_columns = lax.broadcasted_iota(jnp.int32, (tokens_here, n * cap), 1)
    place[...] = (slot_columns == columns[:, 0:1].astype(jnp.int32)).astype(jnp.bfloat16)

    for load in loads:
        load.wait()
    for share in shares:
        share.wait_recv()

    @pl.loop(0, 4)
    def _(turn):
        chunk = 3 - (2 * turn) % 4 - turn // 2
        first = chunk * quarter

        @pl.loop(0, quarter)
        def _(k):
            @pl.when(first + k > 0)
            def _():
                dispatch(first + k).wait_recv()

        here = pl.ds(pl.multiple_of(chunk * rows, rows), rows)
        total[...] = jnp.zeros_like(total)

        @pl.loop(0, 2 * (hidden // TILE))
        def _(piece):
            part = piece // (hidden // TILE)
            cut = pl.ds(pl.multiple_of((piece % (hidden // TILE)) * TILE, TILE), TILE)
            middle = jnp.dot(
                received[here, :], full_in[part, :, cut], preferred_element_type=jnp.float32
            )
            middle = jnp.maximum(middle, 0.0).astype(jnp.bfloat16)
            total[...] += jnp.dot(
                middle, full_out[part, cut, :], preferred_element_type=jnp.float32
            )

        result[here, :] = total[...].astype(jnp.bfloat16)

        @pl.loop(0, quarter)
        def _(k):
            @pl.when(first + k > 0)
            def _():
                give_back(first + k).start()

            @pl.when(first + k == 0)
            def _():
                returned[block(0), :] = result[block(0), :]

    arrived = jnp.zeros((tokens_here, width), jnp.float32)
    for chunk in (1, 3, 0, 2):
        for slot in range(chunk * quarter, (chunk + 1) * quarter):
            if slot > 0:
                give_back(slot).wait_recv()
        here = pl.ds(chunk * rows, rows)
        arrived += jnp.dot(
            place[:, here], returned[here, :], preferred_element_type=jnp.float32
        )
    mixed = tokens_ref[...].astype(jnp.float32) + columns[:, 1:2] * arrived
    out_ref[...] = mixed.astype(jnp.bfloat16)

    @pl.loop(1, n)
    def _(slot):
        dispatch(slot).wait_send()
        give_back(slot).wait_send()

    for share in shares:
        share.wait_send()


def in_one_kernel(n, tokens, expert_ids, slot_ids, centroids, w_in, w_out):
    count, width = tokens.shape
    cap = 2 * count // n
    slots = n * cap
    rows = slots // 4
    hidden = w_in.shape[2]
    vmem = pl.BlockSpec(memory_space=pltpu.VMEM)
    hbm = pl.BlockSpec(memory_space=pl.ANY)
    sems = pltpu.SemaphoreType.DMA
    return pl.pallas_call(
        functools.partial(expert_kernel, n, cap),
        out_shape=pltpu.VMEM((count, width), jnp.bfloat16),
        in_specs=[vmem, vmem, hbm, vmem, hbm, hbm],
        out_specs=vmem,
        scratch_shapes=[
            pltpu.VMEM((slots, width), jnp.bfloat16),
            pltpu.VMEM((slots, width), jnp.bfloat16),
            pltpu.VMEM((slots, width), jnp.bfloat16),
            pltpu.VMEM((slots, width), jnp.bfloat16),
            pltpu.VMEM((rows, width), jnp.float32),
            pltpu.VMEM((count, width), jnp.bfloat16),
            pltpu.VMEM((count, slots), jnp.bfloat16),
            pltpu.VMEM((count, 128), jnp.float32),
            pltpu.VMEM((2, width, hidden), jnp.bfloat16),
            pltpu.VMEM((2, hidden, width), jnp.bfloat16),
            sems((3,)),
            sems((2,)),
            sems((2,)),
            sems((n,)),
            sems((n,)),
            sems((n,)),
            sems((n,)),
        ],
        compiler_params=pltpu.CompilerParams(
            collective_id=0, has_side_effects=True, vmem_limit_bytes=60 * 1024 * 1024
        ),
    )(
        expert_ids.reshape(1, count),
        slot_ids.reshape(1, count),
        tokens,
        centroids,
        w_in,
        w_out,
    )


def in_plain_ops(tokens, expert_ids, slot_ids, centroids, w_in, w_out):
    experts = centroids.shape[0]
    count_rows = tokens.shape[0]
    model_width = tokens.shape[1]
    capacity = 2 * count_rows // experts
    buffer_rows = expert_ids * capacity + slot_ids
    outgoing = (
        jnp.zeros((experts * capacity, model_width), jnp.bfloat16).at[buffer_rows].set(tokens)
    )
    outgoing = outgoing.reshape(experts, capacity, model_width)
    scores = jnp.dot(tokens, centroids.T, preferred_element_type=jnp.float32)
    columns = jnp.arange(experts, dtype=jnp.int32)
    chosen = jnp.sum(jnp.where(columns[None, :] == expert_ids[:, None], scores, 0.0), axis=1)
    gating = jax.nn.sigmoid(chosen)
    full_in, full_out = (
        lax.all_gather(w_in, "grp", axis=2, tiled=True),
        lax.all_gather(w_out, "grp", axis=1, tiled=True),
    )
    received = lax.all_to_all(outgoing, "ex", split_axis=0, concat_axis=0, tiled=True)
    flat_rows = received.reshape(-1, model_width)
    hidden = jnp.maximum(
        jnp.dot(flat_rows, full_in[0], preferred_element_type=jnp.float32), 0.0
    ).astype(jnp.bfloat16)
    result = jnp.dot(hidden, full_out[0], preferred_element_type=jnp.float32)
    returned = lax.all_to_all(
        result.astype(jnp.bfloat16).reshape(received.shape),
        "ex",
        split_axis=0,
        concat_axis=0,
        tiled=True,
    )
    arrived = returned.reshape(-1, model_width)[buffer_rows]
    mixed_rows = tokens.astype(jnp.float32) + gating[:, None] * arrived.astype(jnp.float32)
    return mixed_rows.astype(jnp.bfloat16)


def solution(mesh):
    n = mesh.shape["ex"]

    def on_device(tokens, expert_ids, slot_ids, centroids, w_in, w_out):
        capacity = 2 * tokens.shape[0] // n
        if mesh.shape["grp"] == 2 and n % 4 == 0 and capacity % 16 == 0:
            return in_one_kernel(n, tokens, expert_ids, slot_ids, centroids, w_in, w_out)
        return in_plain_ops(tokens, expert_ids, slot_ids, centroids, w_in, w_out)

    in_specs = (
        P(("grp", "ex"), None),
        P(("grp", "ex")),
        P(("grp", "ex")),
        P(),
        P("ex", None, "grp"),
        P("ex", "grp", None),
    )
    out_specs = P(("grp", "ex"), None)
    return jax.shard_map(
        on_device, mesh=mesh, in_specs=in_specs, out_specs=out_specs, check_vma=False
    )
```
